128 devices in a mesh: strike: 16 (over z_hi, y, core), dip: 8 (over x, z_lo).
Axes of the slice: x: 4, y: 4, z: 4 (z_hi: 2, z_lo: 2; z = z_hi * 2 + z_lo), core: 2. Of those that a mesh axis runs over, the one named last changes fastest.
Arguments:
- slip: float32 [8192, 2048], P('strike', 'dip'), may hold values from -4 to 8
- slip_rate: float32 [8192, 2048], P('strike', 'dip'), may hold values from -6 to 6
- state: float32 [8192, 2048], P('strike', 'dip'), may hold values from -1 to 1
- loading: float32 [8192, 2048], P('strike', 'dip'), may hold values from -8 to 8
- normal_stress: float32 [8192, 2048], P('strike', 'dip'), may hold values from 0.5 to 2
- patch: int32 [8192, 2048], P('strike', 'dip'), may hold values from 0 to 3
- rate_coef: float32 [4], replicated, may hold values from 0.3 to 1
- state_coef: float32 [4], replicated, may hold values from 0.3 to 1
- slip_scale: float32 [4], replicated, may hold values from 0.5 to 2
- kernel: bfloat16 [16, 2048, 8192], P(None, ('strike', 'dip')), may hold values from -1.5 to 1.5
- history: bfloat16 [16, 2, 2048, 8192], P(None, None, ('strike', 'dip')), may hold values from -6 to 6
Outputs:
- new_rate: float32 [8192, 2048], P('strike', 'dip')
- new_state: float32 [8192, 2048], P('strike', 'dip')
- transfer_stress: float32 [8192, 2048], P('strike', 'dip')
- rate_modes: bfloat16 [2, 2048, 8192], P(None, ('strike', 'dip'))
The draws below stay inside these ranges and needn't reach their ends.
All inputs are finite; a program needn't handle non-finite values.
Results may differ from the reference program's by a relative error of at most 0.001.
Values sent between devices are 32-bit elements; how exact they have to be, the bound alone decides.
No kernel may reach another device: no remote copies, remote signals or barrier semaphores. Data moves between devices by JAX's collectives and lax.ppermute only.
A program may use at most 128 MiB of HBM per device.

```python
import math
import jax
import jax.numpy as jnp

NX = 8192
NY = 2048
HIST = 16
PATCHES = 4
NEWTON = 8


def draw_slip(key, part):
    base = jax.random.fold_in(key, 4711)
    keys = jax.random.split(base, 6)
    along_x = jnp.arange(NX, dtype=jnp.float32)[:, None] / NX
    along_y = jnp.arange(NY, dtype=jnp.float32)[None, :] / NY
    wave_a = jax.random.randint(keys[0], (), 1, 4).astype(jnp.float32)
    wave_b = jax.random.randint(keys[1], (), 1, 3).astype(jnp.float32)
    phase_a = jax.random.uniform(keys[2], (), jnp.float32, 0.0, 2.0 * math.pi)
    phase_b = jax.random.uniform(keys[3], (), jnp.float32, 0.0, 2.0 * math.pi)
    rough = jnp.clip(jax.random.normal(keys[4], (NX, NY), jnp.float32), -4.0, 4.0)
    level = jax.random.uniform(keys[5], (), jnp.float32, 1.5, 2.5)
    amp_a = 0.8
    amp_b = 0.5
    smooth = level + amp_a * jnp.cos(2.0 * math.pi * wave_a * along_x + phase_a) + amp_b * jnp.cos(2.0 * math.pi * wave_b * along_y + phase_b)
    return (rough + smooth).astype(jnp.float32)


def with_ends(values, rng, low, high):
    index_at = [jax.random.randint(jax.random.fold_in(rng, axis), (), 0, length) for axis, length in enumerate(values.shape)]
    longest = values.shape.index(max(values.shape))
    beside = index_at[:longest] + [(index_at[longest] + 1) % values.shape[longest]] + index_at[longest + 1:]
    return values.at[tuple(index_at)].set(low).at[tuple(beside)].set(high)


def steps_of(key, shape, cuts, low, largest):
    loudness = 1.0
    for dim, parts in cuts:
        steps = jax.random.uniform(jax.random.fold_in(jax.random.fold_in(key, 6), dim), (parts,), jnp.float32, low / len(cuts), largest / len(cuts))
        loudness = loudness * jnp.repeat(jnp.exp(steps), shape[dim] // parts).reshape((-1,) + (1,) * (len(shape) - 1 - dim))
    return loudness


def bell_draw(key, extent, width, most, cuts=(), kind=jnp.bfloat16):
    entries = width * jax.random.normal(key, extent, jnp.float32)
    if cuts:
        entries = entries * steps_of(key, extent, cuts, -0.22, 0.18)
    return jnp.clip(entries, -most, most).astype(kind)


def setup_inputs(seed: int = 0) -> dict:
    splits = jax.random.split(jax.random.key(seed), 12)
    return {
        "slip": draw_slip(jax.random.fold_in(splits[11], 71), 0),
        "slip_rate": bell_draw(splits[1], (NX, NY), 1.0, 6.0, ((0, 16), (1, 8)), jnp.float32),
        "state": jnp.clip(jax.random.uniform(splits[2], (NX, NY), jnp.float32, -1.0, 1.0) * steps_of(splits[2], (NX, NY), ((0, 16), (1, 8)), -0.4, 0.0), -1.0, 1.0),
        "loading": bell_draw(splits[3], (NX, NY), 2.0, 8.0, ((0, 16), (1, 8)), jnp.float32),
        "normal_stress": jnp.clip(jnp.exp(math.log(2.0) - 1.3862944 * jax.random.uniform(splits[4], (NX, NY), jnp.float32) ** steps_of(splits[4], (NX, NY), ((0, 16), (1, 8)), -0.2, 0.2)), 0.5, 2.0),
        "patch": with_ends(jax.random.randint(splits[5], (NX, NY), 0, PATCHES), jax.random.fold_in(splits[5], 1), 0, PATCHES - 1).astype(jnp.int32),
        "rate_coef": jnp.clip(jnp.exp(jax.random.uniform(splits[6], (PATCHES,), jnp.float32, math.log(0.3), math.log(1.0))), 0.3, 1.0),
        "state_coef": jnp.clip(jnp.exp(jax.random.uniform(splits[7], (PATCHES,), jnp.float32, math.log(0.3), math.log(1.0))), 0.3, 1.0),
        "slip_scale": jnp.clip(jnp.exp(jax.random.uniform(splits[8], (PATCHES,), jnp.float32, math.log(0.5), math.log(2.0))), 0.5, 2.0),
        "kernel": bell_draw(splits[9], (HIST, NY, NX), HIST ** -0.5, 1.5, ((1, 128),)),
        "history": bell_draw(splits[10], (HIST, 2, NY, NX), 1.0, 6.0, ((2, 128),)),
    }


shear_modulus = 1.0
damping = 0.5
relaxation = 0.35
time_step = 0.1

def inverse_sinh(value):
    size_v = jnp.abs(value)
    square = size_v * size_v
    result = jnp.log1p(size_v + square / (1.0 + jnp.sqrt(square + 1.0)))
    return jnp.where(value < 0.0, -result, result)

def lookup(patch, table):
    result = jnp.zeros(patch.shape, jnp.float32)
    for label in range(PATCHES):
        result = jnp.where(patch == label, table[label], result)
    return result

def friction(slip_rate, state, loading, normal_stress, transfer, coef_a, coef_b, length_l):
    stress = loading + transfer
    prefix = 2.0 * jnp.exp(-state / coef_a)
    angle_w = inverse_sinh(slip_rate / prefix)
    for iteration in range(NEWTON):
        residue = normal_stress * coef_a * angle_w + damping * prefix * jnp.sinh(angle_w) - stress
        slope = normal_stress * coef_a + damping * prefix * jnp.cosh(angle_w)
        ratio = residue / slope
        angle_w = angle_w - relaxation * ratio / (1.0 + jnp.abs(ratio))
    new_rate = prefix * jnp.sinh(angle_w)
    new_state = state + time_step * (coef_b / length_l) * (jnp.exp(-state / coef_b) - jnp.abs(new_rate))
    return (new_rate, new_state)

def wavenumber(count):
    index = jnp.arange(count, dtype=jnp.int32)
    return 2.0 * math.pi / count * ((index + count // 2) % count - count // 2).astype(jnp.float32)

def reference(slip, slip_rate, state, loading, normal_stress, patch, rate_coef, state_coef, slip_scale, kernel, history):
    slip_hat = jnp.fft.fft2(slip, norm='ortho').T
    rate_hat = jnp.fft.fft2(slip_rate, norm='ortho').T
    wave_x = wavenumber(NX)
    wave_y = wavenumber(NY)
    magnitude = jnp.sqrt(wave_y[:, None] ** 2 + wave_x[None, :] ** 2)
    kernel_full = kernel.astype(jnp.float32)
    memory_re = jnp.einsum('jrc,jrc->rc', kernel_full, history[:, 0].astype(jnp.float32))
    memory_im = jnp.einsum('jrc,jrc->rc', kernel_full, history[:, 1].astype(jnp.float32))
    static = -0.5 * shear_modulus * magnitude
    stress_re = static * jnp.real(slip_hat).astype(jnp.float32) + memory_re
    stress_im = static * jnp.imag(slip_hat).astype(jnp.float32) + memory_im
    stress_hat = (stress_re + 1j * stress_im).T
    transfer = jnp.real(jnp.fft.ifft2(stress_hat, norm='ortho')).astype(jnp.float32)
    rate_modes = jnp.stack([jnp.real(rate_hat), jnp.imag(rate_hat)]).astype(jnp.bfloat16)
    coef_a = lookup(patch, rate_coef)
    coef_b = lookup(patch, state_coef)
    length_l = lookup(patch, slip_scale)
    new_rate, new_state = friction(slip_rate, state, loading, normal_stress, transfer, coef_a, coef_b, length_l)
    return (new_rate, new_state, transfer, rate_modes)
```

```python
import functools
import math

import jax
import jax.numpy as jnp
import numpy as np
from jax import lax
from jax.experimental import pallas as pl
from jax.experimental.pallas import tpu as pltpu
from jax.sharding import PartitionSpec as P

NEWTON = 8
NX = 8192
NY = 2048
HIST = 16
BAND = 16
SLOTS = 8
SENT = BAND + SLOTS
LANES = 128

relaxation = 0.35
time_step = 0.1
f32 = jnp.float32
bf16 = jnp.bfloat16


def halves(table):
    high = table.astype(np.float32).astype(bf16)
    low = (table - high.astype(np.float64)).astype(np.float32).astype(bf16)
    return jnp.asarray(high), jnp.asarray(low)


def wave(rows, cols, modulus, sign):
    product = np.outer(np.arange(rows), np.arange(cols)) % modulus
    angles = 2.0 * math.pi / modulus * product
    return np.cos(angles), sign * np.sin(angles)


def right_table(sign, scale):
    co, si = wave(LANES, LANES, LANES, sign)
    return halves(scale * np.block([[co, si], [-si, co]]))


def left_table(sign):
    co, si = wave(64, 64, 64, sign)
    return halves(np.block([[co, -si], [si, co]]))


def plain(pair):
    return jnp.asarray(np.stack(pair).astype(np.float32))


def split(x):
    high = x.astype(bf16)
    low = (x - high.astype(f32)).astype(bf16)
    return high, low


def dot(a, b):
    return jnp.dot(a, b, preferred_element_type=f32)


def cadd(a, b):
    im = a[1] if b[1] is None else b[1] if a[1] is None else a[1] + b[1]
    return (a[0] + b[0], im)


def csub_conj(a, b):
    im = b[1] if a[1] is None else None if b[1] is None else b[1] - a[1]
    if a[1] is not None and b[1] is None:
        im = -a[1]
    return (a[0] - b[0], im)


def cturn(a, k, n, sign):
    if k == 0:
        return a
    re, im = a
    if 4 * k == n:
        if im is None:
            return (None, re * sign if sign < 0 else re)
        return (-sign * im, sign * re)
    co = math.cos(2 * math.pi * k / n)
    si = sign * math.sin(2 * math.pi * k / n)
    if im is None:
        return (co * re, si * re)
    if 8 * k == n:
        return (co * (re - sign * im), co * (im + sign * re))
    return (co * re - si * im, si * re + co * im)


def real_dft(values):
    n = len(values)
    if n == 1:
        return [(values[0], None)]
    even, odd = real_dft(values[::2]), real_dft(values[1::2])
    out = [None] * (n // 2 + 1)
    for k in range(n // 4 + 1):
        if 4 * k == n:
            re = even[k][0]
            out[k] = (re, -odd[k][0])
            continue
        turned = cturn(odd[k], k, n, -1.0)
        out[k] = cadd(even[k], turned)
        out[n // 2 - k] = csub_conj(even[k], turned)
    return out


def real_inverse(modes):
    n = 2 * (len(modes) - 1)
    if n == 1 or len(modes) == 1:
        return [modes[0][0]]
    if n == 2:
        return [modes[0][0] + modes[1][0], modes[0][0] - modes[1][0]]
    even, odd = [], []
    for k in range(n // 4 + 1):
        a, b = modes[k], modes[n // 2 - k]
        if k == 0:
            even.append((a[0] + b[0], None))
            odd.append((a[0] - b[0], None))
        elif 4 * k == n:
            even.append((2.0 * a[0], None))
            odd.append((-2.0 * a[1], None))
        else:
            even.append((a[0] + b[0], a[1] - b[1]))
            odd.append(cturn((a[0] - b[0], a[1] + b[1]), k, n, 1.0))
    first, second = real_inverse(even), real_inverse(odd)
    out = []
    for one, two in zip(first, second):
        out += [one, two]
    return out


def dip_forward(x_ref, turn_ref, hi_ref, lo_ref, out_ref, a_hi, a_lo, prod):
    def fill(first_row, base, count):
        def body(step, carry):
            row = pl.multiple_of(first_row + step * 16, 16)
            tiles = []
            for part in range(8):
                for half in range(2):
                    tiles.append(x_ref[part, pl.ds(row, 16), half * LANES:(half + 1) * LANES])
            modes = real_dft(tiles)
            for q in range(count):
                re, im = modes[q] if q <= 8 else modes[16 - q]
                if im is not None and q > 8:
                    im = -im
                co, si = turn_ref[0, q:q + 1, :], turn_ref[1, q:q + 1, :]
                if q == 0:
                    new_re, new_im = re, jnp.zeros_like(re)
                elif im is None:
                    new_re, new_im = re * co, re * si
                else:
                    new_re, new_im = re * co - im * si, re * si + im * co
                at = pl.multiple_of((base + q) * 64 + step * 16, 16)
                for c, value in enumerate((new_re, new_im)):
                    high, low = split(value)
                    a_hi[pl.ds(at, 16), c * LANES:(c + 1) * LANES] = high
                    a_lo[pl.ds(at, 16), c * LANES:(c + 1) * LANES] = low
            return carry

        lax.fori_loop(0, 4, body, 0)

    fill(0, 0, 9)
    fill(64, 9, 16)
    w_hi, w_lo = hi_ref[...], lo_ref[...]
    for start, stop in ((0, 9), (9, 25)):
        rows = pl.ds(start * 64, (stop - start) * 64)
        prod[rows, :] = dot(a_hi[rows, :], w_hi) + dot(a_lo[rows, :], w_hi) + dot(a_hi[rows, :], w_lo)

    def turned(group):
        rows = pl.ds(group * 64, 64)
        both = jnp.concatenate([prod[rows, :LANES], prod[rows, LANES:]], axis=0)
        return both.T

    zero_row = turned(0)
    mixed = jnp.concatenate([turned(8)[:64], zero_row[64:]], axis=0)
    out_ref[pl.ds(BAND, LANES, stride=SENT), :] = mixed
    for q in range(1, 8):
        out_ref[pl.ds(BAND + q, LANES, stride=SENT), :] = turned(q)
    row = lax.broadcasted_iota(jnp.int32, (LANES, LANES), 0)
    lane = lax.broadcasted_iota(jnp.int32, (LANES, LANES), 1)
    moved = pltpu.roll(zero_row, 64, axis=1)
    rate_zero = jnp.where((row == 0) & (lane >= 64), moved, turned(9))
    out_ref[pl.ds(0, LANES, stride=SENT), :] = rate_zero
    for q in range(1, 16):
        out_ref[pl.ds(q, LANES, stride=SENT), :] = turned(9 + q)


def strike_rows(rows, turn_ref, ahi_ref, alo_ref, mhi_ref, mlo_ref, a_hi, a_lo, b_hi, b_lo):
    count = len(rows)
    for r, x in enumerate(rows):
        flat = x.T
        both = jnp.concatenate([flat[:64], flat[64:]], axis=1)
        high, low = split(both)
        a_hi[r * 64:(r + 1) * 64, :] = high
        a_lo[r * 64:(r + 1) * 64, :] = low
    size = count * 64
    w_hi, w_lo = ahi_ref[...], alo_ref[...]
    x_hi, x_lo = a_hi[:size, :], a_lo[:size, :]
    prod = dot(x_hi, w_hi) + dot(x_lo, w_hi) + dot(x_hi, w_lo)
    co, si = turn_ref[0], turn_ref[1]
    for r in range(count):
        re, im = prod[r * 64:(r + 1) * 64, :LANES], prod[r * 64:(r + 1) * 64, LANES:]
        new = jnp.concatenate([re * co - im * si, re * si + im * co], axis=0)
        high, low = split(new)
        b_hi[:, r * LANES:(r + 1) * LANES] = high
        b_lo[:, r * LANES:(r + 1) * LANES] = low
    width = count * LANES
    m_hi, m_lo = mhi_ref[...], mlo_ref[...]
    return dot(m_hi, b_hi[:, :width]) + dot(m_hi, b_lo[:, :width]) + dot(m_lo, b_hi[:, :width])


def stress_kernel(slip_ref, rate_ref, mem_ref, wave_ref, kx_ref, turn_ref, ahi_ref, alo_ref, mhi_ref, mlo_ref,
                  back_turn_ref, bhi_ref, blo_ref, nhi_ref, nlo_ref, out_ref, a_hi, a_lo, b_hi, b_lo, prod):
    rows = [slip_ref[:, q, :] for q in range(SLOTS)]
    lane = lax.broadcasted_iota(jnp.int32, (LANES, LANES), 1)
    special = jnp.where(lane < 64, pltpu.roll(rate_ref[:, 0, :], 64, axis=1), 0.0)
    rows.append(special)
    hat = strike_rows(rows, turn_ref, ahi_ref, alo_ref, mhi_ref, mlo_ref, a_hi, a_lo, b_hi, b_lo)
    kx2 = kx_ref[...]

    def static(b):
        return -0.5 * jnp.sqrt(wave_ref[b:b + 1, :] + kx2)

    def weighted(b, value):
        return jnp.concatenate([b, b], axis=0) * value

    w_zero, w_special, w_eight = wave_ref[16:17, :], wave_ref[17:18, :], wave_ref[18:19, :]
    for b in range(BAND):
        stress = mem_ref[b]
        if b == 0:
            slot = w_zero * hat[:, :LANES] + w_special * hat[:, 8 * LANES:]
            stress = stress + weighted(static(0), slot)
        elif b == 8:
            stress = stress + weighted(static(8), w_eight * hat[:, :LANES])
        elif b < 8:
            stress = stress + weighted(2.0 * static(b), hat[:, b * LANES:(b + 1) * LANES])
        high, low = split(stress)
        b_hi[:, b * LANES:(b + 1) * LANES] = high
        b_lo[:, b * LANES:(b + 1) * LANES] = low
    n_hi, n_lo = nhi_ref[...], nlo_ref[...]
    lines = dot(n_hi, b_hi[...]) + dot(n_hi, b_lo[...]) + dot(n_lo, b_hi[...])
    co, si = back_turn_ref[0], back_turn_ref[1]
    for b in range(BAND):
        re, im = lines[:64, b * LANES:(b + 1) * LANES], lines[64:, b * LANES:(b + 1) * LANES]
        for c, value in enumerate((re * co - im * si, re * si + im * co)):
            high, low = split(value)
            a_hi[b * 64:(b + 1) * 64, c * LANES:(c + 1) * LANES] = high
            a_lo[b * 64:(b + 1) * 64, c * LANES:(c + 1) * LANES] = low
    w_hi, w_lo = bhi_ref[...], blo_ref[...]
    prod[...] = dot(a_hi[...], w_hi) + dot(a_lo[...], w_hi) + dot(a_hi[...], w_lo)
    for b in range(BAND):
        both = jnp.concatenate([prod[b * 64:(b + 1) * 64, :LANES], prod[b * 64:(b + 1) * 64, LANES:]], axis=0)
        out_ref[pl.ds(b, LANES, stride=BAND), :] = both.T


def modes_kernel(rate_ref, keep_ref, turn_ref, ahi_ref, alo_ref, mhi_ref, mlo_ref, out_ref, a_hi, a_lo, b_hi, b_lo, flat):
    rows = [rate_ref[:, b, :] for b in range(BAND)]
    rows[0] = rows[0] * keep_ref[...]
    hat = strike_rows(rows, turn_ref, ahi_ref, alo_ref, mhi_ref, mlo_ref, a_hi, a_lo, b_hi, b_lo)
    for b in range(BAND):
        flat[b * LANES:(b + 1) * LANES, :] = hat[:, b * LANES:(b + 1) * LANES]
    for c in range(2):
        for p in range(64):
            line = flat[pl.ds(c * 64 + p, BAND, stride=LANES), :]
            out_ref[c, :, p * LANES:(p + 1) * LANES] = line.astype(bf16)


def dip_inverse(x_ref, turn_ref, hi_ref, lo_ref, out_ref, a_hi, a_lo, prod):
    for b in range(BAND):
        flat = x_ref[pl.ds(b, LANES, stride=BAND), :].T
        both = jnp.concatenate([flat[:64], flat[64:]], axis=1)
        high, low = split(both)
        a_hi[b * 64:(b + 1) * 64, :] = high
        a_lo[b * 64:(b + 1) * 64, :] = low
    w_hi, w_lo = hi_ref[...], lo_ref[...]
    prod[...] = dot(a_hi[...], w_hi) + dot(a_lo[...], w_hi) + dot(a_hi[...], w_lo)

    def body(step, carry):
        line = []
        for b in range(BAND):
            at = pl.multiple_of(b * 64 + step * 8, 8)
            re, im = prod[pl.ds(at, 8), :LANES], prod[pl.ds(at, 8), LANES:]
            if b:
                co, si = turn_ref[0, b:b + 1, :], turn_ref[1, b:b + 1, :]
                re, im = re * co - im * si, re * si + im * co
            line.append((re, im))
        modes = [(2.0 * line[0][0], None)]
        for b in range(1, 8):
            modes.append((line[b][0] + line[16 - b][0], line[b][1] - line[16 - b][1]))
        modes.append((2.0 * line[8][0], None))
        cells = real_inverse(modes)
        row = pl.multiple_of(step * 8, 8)
        for j in range(16):
            out_ref[j // 2, pl.ds(row, 8), (j % 2) * LANES:(j % 2 + 1) * LANES] = cells[j]
        return carry

    lax.fori_loop(0, 8, body, 0)


def memory_kernel(kernel_ref, history_ref, out_ref):
    step = pl.program_id(0)
    for p in range(8):
        lanes = slice(p * LANES, (p + 1) * LANES)
        sums = [jnp.zeros((BAND, LANES), f32), jnp.zeros((BAND, LANES), f32)]
        for lag in range(HIST):
            factor = kernel_ref[lag, :, lanes].astype(f32)
            for c in range(2):
                sums[c] = sums[c] + factor * history_ref[lag, c, :, lanes].astype(f32)
        for c in range(2):
            out_ref[pl.ds(c * 64 + step * 8 + p, BAND, stride=LANES), :] = sums[c]


def friction_first(rate_ref, state_ref, normal_ref, patch_ref, a_ref, b_ref, l_ref,
                   stiff_ref, half_ref, w_ref, base_ref, gain_ref):
    patch, state = patch_ref[...], state_ref[...]

    def look(table):
        result = jnp.full(patch.shape, table[0], f32)
        for label in range(1, 4):
            result = jnp.where(patch == label, table[label], result)
        return result

    coef_a, coef_b, length_l = look(a_ref), look(b_ref), look(l_ref)
    half = jnp.exp(-state / coef_a)
    value = rate_ref[...] / (2.0 * half)
    size = jnp.abs(value)
    square = size * size
    result = jnp.log1p(size + square / (1.0 + jnp.sqrt(square + 1.0)))
    w_ref[...] = jnp.where(value < 0.0, -result, result)
    stiff_ref[...] = normal_ref[...] * coef_a
    half_ref[...] = half
    gain = time_step * (coef_b / length_l)
    gain_ref[...] = gain
    base_ref[...] = state + gain * jnp.exp(-state / coef_b)


def friction_second(transfer_ref, loading_ref, stiff_ref, half_ref, w_ref, base_ref, gain_ref,
                    rate_out, state_out, transfer_out):
    transfer = transfer_ref[...]
    transfer_out[...] = transfer
    stress = loading_ref[...] + transfer
    stiff, half, w = stiff_ref[...], 0.5 * half_ref[...], w_ref[...]

    def powers(w):
        up = jnp.exp(w)
        return half * up, half / up

    for _ in range(NEWTON):
        up, down = powers(w)
        residue = stiff * w + (up - down) - stress
        slope = stiff + (up + down)
        w = w - relaxation * residue / (slope + jnp.abs(residue))
    up, down = powers(w)
    new_rate = 2.0 * (up - down)
    rate_out[...] = new_rate
    state_out[...] = base_ref[...] - gain_ref[...] * jnp.abs(new_rate)


def sds(shape, dtype=f32):
    return jax.ShapeDtypeStruct(shape, dtype)


def params():
    return pltpu.CompilerParams(vmem_limit_bytes=56 << 20)


def whole(kernel, out, scratch, name, flops=0):
    return pl.pallas_call(
        kernel, out_shape=out, scratch_shapes=scratch, compiler_params=params(), name=name,
        cost_estimate=pl.CostEstimate(flops=flops, transcendentals=0, bytes_accessed=2 << 20))


def per_device(slip, slip_rate, state, loading, normal_stress, patch, rate_coef, state_coef, slip_scale, kernel, history):
    axes = ("strike", "dip")
    index = lax.axis_index("strike") * lax.axis_size("dip") + lax.axis_index("dip")

    cells = jnp.concatenate([slip.reshape(8, 64, 256), slip_rate.reshape(8, 64, 256)], axis=1)
    cells = lax.all_to_all(cells, "dip", split_axis=0, concat_axis=0, tiled=True)

    memory = pl.pallas_call(
        memory_kernel, grid=(8,),
        in_specs=[pl.BlockSpec((HIST, BAND, 1024), lambda i: (0, 0, i)),
                  pl.BlockSpec((HIST, 2, BAND, 1024), lambda i: (0, 0, 0, i))],
        out_specs=pl.BlockSpec((BAND * LANES, LANES), lambda i: (0, 0)),
        out_shape=sds((BAND * LANES, LANES)), compiler_params=params(), name="memory",
        cost_estimate=pl.CostEstimate(flops=10_000_000_000, transcendentals=0, bytes_accessed=13 << 20),
    )(kernel, history).reshape(BAND, LANES, LANES)

    smem = pl.BlockSpec(memory_space=pltpu.SMEM)
    block = pl.BlockSpec((128, 256), lambda i: (i, 0))
    stiff, half, start_w, base, gain = pl.pallas_call(
        friction_first, grid=(4,), in_specs=[block] * 4 + [smem] * 3, out_specs=[block] * 5,
        out_shape=[sds((512, 256))] * 5, compiler_params=params(), name="friction_first",
        cost_estimate=pl.CostEstimate(flops=5_000_000_000, transcendentals=0, bytes_accessed=5 << 20),
    )(slip_rate, state, normal_stress, patch, rate_coef, state_coef, slip_scale)

    turn = plain(wave(BAND, LANES, NY, -1.0))
    hi, lo = right_table(-1.0, 1.0 / math.sqrt(NY))
    sent = whole(
        dip_forward, sds((LANES * SENT, LANES)),
        [pltpu.VMEM((25 * 64, 256), bf16), pltpu.VMEM((25 * 64, 256), bf16), pltpu.VMEM((25 * 64, 256), f32)],
        "dip_forward")(cells, turn, hi, lo)
    rows = lax.all_to_all(sent.reshape(LANES, SENT, LANES), axes, split_axis=0, concat_axis=0, tiled=True)

    band = index * BAND + jnp.arange(BAND, dtype=jnp.int32)
    wave_y = 2.0 * math.pi / NY * ((band + NY // 2) % NY - NY // 2).astype(f32)
    upper = index >= 64
    weights = jnp.stack([
        jnp.where(upper, jnp.where(index == 64, 1.0, 2.0), 0.0),
        jnp.where(index == 0, 1.0, 0.0),
        jnp.where(upper, 0.0, 2.0)])
    wave_rows = jnp.broadcast_to(
        jnp.concatenate([wave_y * wave_y, weights, jnp.zeros((5,), f32)])[:, None], (24, LANES))
    wave_x = 2.0 * math.pi / NX * ((np.arange(NX) + NX // 2) % NX - NX // 2)
    kx2 = jnp.asarray((wave_x.astype(np.float32) ** 2).reshape(64, LANES))
    keep = jnp.where((index == 0) & (jnp.arange(LANES) >= 64), 0.0, 1.0)[None, :]

    turn_x = plain(wave(64, LANES, NX, -1.0))
    turn_back = plain(wave(64, LANES, NX, 1.0))
    a_hi, a_lo = right_table(-1.0, 1.0 / math.sqrt(NX))
    m_hi, m_lo = left_table(-1.0)
    b_hi, b_lo = right_table(1.0, 1.0 / math.sqrt(NX))
    n_hi, n_lo = left_table(1.0)

    def full(shape):
        return pl.BlockSpec(shape, lambda i: (0,) * len(shape))

    square = [full((256, 256))] * 2 + [full((LANES, LANES))] * 2
    lines = pl.pallas_call(
        stress_kernel, grid=(1,),
        in_specs=[pl.BlockSpec((LANES, 8, LANES), lambda i: (0, 2, 0)),
                  pl.BlockSpec((LANES, 8, LANES), lambda i: (0, 0, 0)),
                  full((BAND, LANES, LANES)), full((24, LANES)), full((64, LANES)),
                  full((2, 64, LANES))] + square + [full((2, 64, LANES))] + square,
        out_specs=full((LANES * BAND, LANES)),
        out_shape=sds((LANES * BAND, LANES)),
        scratch_shapes=[pltpu.VMEM((1024, 256), bf16), pltpu.VMEM((1024, 256), bf16),
                        pltpu.VMEM((LANES, 2048), bf16), pltpu.VMEM((LANES, 2048), bf16),
                        pltpu.VMEM((1024, 256), f32)],
        compiler_params=params(), name="stress",
        cost_estimate=pl.CostEstimate(flops=1_000_000, transcendentals=0, bytes_accessed=4 << 20),
    )(rows, rows, memory, wave_rows, kx2, turn_x, a_hi, a_lo, m_hi, m_lo, turn_back, b_hi, b_lo, n_hi, n_lo)
    lines = lax.all_to_all(lines.reshape(LANES, BAND, LANES), axes, split_axis=0, concat_axis=0, tiled=True)

    rate_modes = pl.pallas_call(
        modes_kernel, grid=(1,),
        in_specs=[pl.BlockSpec((LANES, BAND, LANES), lambda i: (0, 0, 0)), full((1, LANES)),
                  full((2, 64, LANES))] + square,
        out_specs=full((2, BAND, NX)),
        out_shape=sds((2, BAND, NX), bf16),
        scratch_shapes=[pltpu.VMEM((1024, 256), bf16), pltpu.VMEM((1024, 256), bf16),
                        pltpu.VMEM((LANES, 2048), bf16), pltpu.VMEM((LANES, 2048), bf16),
                        pltpu.VMEM((BAND * LANES, LANES), f32)],
        compiler_params=params(), name="modes",
        cost_estimate=pl.CostEstimate(flops=5_000_000_000, transcendentals=0, bytes_accessed=4 << 20),
    )(rows, keep, turn_x, a_hi, a_lo, m_hi, m_lo)

    turn_y = plain(wave(BAND, LANES, NY, 1.0))
    c_hi, c_lo = right_table(1.0, 0.5 / math.sqrt(NY))
    back = whole(
        dip_inverse, sds((8, 64, 256)),
        [pltpu.VMEM((1024, 256), bf16), pltpu.VMEM((1024, 256), bf16), pltpu.VMEM((1024, 256), f32)],
        "dip_inverse")(lines.reshape(LANES * BAND, LANES), turn_y, c_hi, c_lo)
    transfer = lax.all_to_all(back, "dip", split_axis=0, concat_axis=0, tiled=True).reshape(512, 256)

    new_rate, new_state, transfer = pl.pallas_call(
        friction_second, grid=(4,), in_specs=[block] * 7, out_specs=[block] * 3,
        out_shape=[sds((512, 256))] * 3, compiler_params=params(), name="friction_second",
        cost_estimate=pl.CostEstimate(flops=1_000_000, transcendentals=0, bytes_accessed=5 << 20),
    )(transfer, loading, stiff, half, start_w, base, gain)
    return (new_rate, new_state, transfer, rate_modes)


def solution(mesh):
    cells = P("strike", "dip")
    return jax.shard_map(
        per_device,
        mesh=mesh,
        in_specs=(cells,) * 6 + (P(),) * 3 + (P(None, ("strike", "dip"), None), P(None, None, ("strike", "dip"), None)),
        out_specs=(cells, cells, cells, P(None, ("strike", "dip"), None)),
        check_vma=False,
    )
```
